32 devices in a mesh: gx: 16 (over z, y, core), gy: 2 (over x).
Axes of the slice: x: 2, y: 2, z: 4, core: 2. Of those that a mesh axis runs over, the one named last changes fastest.
Arguments:
- fluid_velocity: float32 [3, 64, 32, 128], P(None, 'gx', 'gy'), may hold values from -6 to 6
- particle_velocity: float32 [16, 2, 4, 3, 128], P('gx', 'gy'), may hold values from -6 to 6
- particle_volume: float32 [16, 2, 4, 128], P('gx', 'gy'), may hold values from 0.02 to 0.3
- satellite_cells: int32 [16, 2, 4, 29, 128], P('gx', 'gy'), may hold values from 0 to 13823, as said below
- live_blocks: int32 [16, 2], P('gx', 'gy'), may hold values from 1 to 4
Outputs:
- void_fraction: float32 [64, 32, 128], P('gx', 'gy')
- drag: float32 [16, 2, 4, 3, 128], P('gx', 'gy')
The draws below stay inside these ranges and needn't reach their ends.
Inputs may be any that keep to these rules, and one draw needn't show every extreme that they name: `satellite_cells`: each entry names a cell of the owning slab's tile of 4 x 16 x 128 cells extended by one layer on each side along x and y, flattened as described in the reference program. `live_blocks`: blocks from this number on hold no live particles.
All inputs are finite; a program needn't handle non-finite values.
Results may differ from the reference program's by a relative error of at most 0.00029.
Values sent between devices are 32-bit elements; how exact they have to be, the bound alone decides.
A program may use at most 64 MiB of HBM per device.

```python
import math
import jax
import jax.numpy as jnp

CX = 4
CY = 16
CZ = 128
BLOCKS = 4
SAT = 29
BLK = 128
NX = 64
NY = 32
NZ = 128
N_GX = 16
N_GY = 2


def draw_satellite_cells(key, part):
    keys = jax.random.split(jax.random.fold_in(key, 11), 6)
    block_shape = (N_GX, N_GY, BLOCKS, 1, 1)
    centre_shape = (3, N_GX, N_GY, BLOCKS, 1, BLK)
    full_shape = (3, N_GX, N_GY, BLOCKS, SAT, BLK)
    cluster_x = jax.random.randint(keys[0], block_shape, 0, CX + 2)
    cluster_y = jax.random.randint(keys[1], block_shape, 0, CY + 2)
    cluster_z = jax.random.randint(keys[2], block_shape, 0, CZ)
    centre_move = jax.random.randint(keys[3], centre_shape, -1, 2)
    offsets = jax.random.randint(keys[4], full_shape, -1, 2)
    moving = (jax.random.randint(keys[5], full_shape, 0, 4) == 0).astype(jnp.int32)
    steps = centre_move + offsets * moving
    layer_x = jnp.clip(cluster_x + steps[0], 0, CX + 1)
    layer_y = jnp.clip(cluster_y + steps[1], 0, CY + 1)
    layer_z = jnp.clip(cluster_z + steps[2], 0, CZ - 1)
    return ((layer_x * (CY + 2) + layer_y) * CZ + layer_z).astype(jnp.int32)


def plant(result, own_key, least, largest):
    index_at = [jax.random.randint(jax.random.fold_in(own_key, axis), (), 0, length) for axis, length in enumerate(result.shape)]
    main_axis = result.shape.index(max(result.shape))
    beside = index_at[:main_axis] + [(index_at[main_axis] + 1) % result.shape[main_axis]] + index_at[main_axis + 1:]
    return result.at[tuple(index_at)].set(least).at[tuple(beside)].set(largest)


def level_of(rng, extent, pieces, least, high):
    loudness = 1.0
    for axis_at, shards_of in pieces:
        heights = jax.random.uniform(jax.random.fold_in(jax.random.fold_in(rng, 6), axis_at), (shards_of,), jnp.float32, least / len(pieces), high / len(pieces))
        loudness = loudness * jnp.repeat(jnp.exp(heights), extent[axis_at] // shards_of).reshape((-1,) + (1,) * (len(extent) - 1 - axis_at))
    return loudness


def normal_values(stream_key, shape, spread, limit, cuts=(), kind=jnp.bfloat16):
    gain = level_of(stream_key, shape, cuts, -0.22, 0.18) if cuts else 1.0
    array = jax.random.normal(stream_key, shape, jnp.float32) * spread * gain
    return jnp.minimum(jnp.maximum(array, -limit), limit).astype(kind)


def setup_inputs(seed: int = 0) -> dict:
    splits = jax.random.split(jax.random.key(seed), 6)
    fluid_velocity = normal_values(splits[0], (3, NX, NY, NZ), 1.0, 6.0, ((1, 16), (2, 2)), jnp.float32)
    particle_velocity = normal_values(splits[1], (N_GX, N_GY, BLOCKS, 3, BLK), 1.0, 6.0, ((0, 16), (1, 2)), jnp.float32)
    particle_volume = jnp.clip(jnp.exp(math.log(0.3) - 2.7080503 * jax.random.uniform(splits[2], (N_GX, N_GY, BLOCKS, BLK), jnp.float32) ** level_of(splits[2], (N_GX, N_GY, BLOCKS, BLK), ((0, 16), (1, 2)), -0.2, 0.2)), 0.02, 0.3)
    satellite_cells = draw_satellite_cells(jax.random.fold_in(splits[5], 71), 0)
    live_blocks = plant(jax.random.randint(splits[4], (N_GX, N_GY), 1, BLOCKS + 1), jax.random.fold_in(splits[4], 1), 1, BLOCKS).astype(jnp.int32)
    return dict(fluid_velocity=fluid_velocity, particle_velocity=particle_velocity, particle_volume=particle_volume, satellite_cells=satellite_cells, live_blocks=live_blocks)


exponent = -2.65
drag_scale = 2.0
void_floor = 0.1


def reference(fluid_velocity, particle_velocity, particle_volume, satellite_cells, live_blocks):
    wide_y = CY + 2
    slab_x = jnp.arange(N_GX, dtype=jnp.int32)[:, None, None, None, None]
    slab_y = jnp.arange(N_GY, dtype=jnp.int32)[None, :, None, None, None]
    layer_x = satellite_cells // (wide_y * CZ)
    layer_y = (satellite_cells // CZ) % wide_y
    layer_z = satellite_cells % CZ
    global_x = (slab_x * CX + layer_x - 1) % NX
    global_y = (slab_y * CY + layer_y - 1) % NY
    flat_cell = ((global_x * NY + global_y) * NZ + layer_z).astype(jnp.int32)
    block_ids = jnp.arange(BLOCKS, dtype=jnp.int32)[None, None, :]
    alive = (block_ids < live_blocks[:, :, None]).astype(jnp.float32)
    volume_share = particle_volume * alive[..., None] / SAT
    weights = jnp.broadcast_to(volume_share[:, :, :, None, :], satellite_cells.shape)
    solid_volume = jnp.zeros((NX * NY * NZ,), jnp.float32).at[flat_cell.reshape(-1)].add(weights.reshape(-1))
    void_flat = jnp.maximum(1.0 - solid_volume, void_floor)
    resistance = void_flat ** exponent
    weight_at = resistance[flat_cell]
    weight_sum = jnp.sum(weight_at, axis=3)
    flow = fluid_velocity.reshape(3, -1)
    forces = []
    for component in range(3):
        pulling = jnp.sum(weight_at * flow[component][flat_cell], axis=3)
        moving = particle_velocity[:, :, :, component, :]
        forces.append(drag_scale * volume_share * (pulling - moving * weight_sum))
    drag = jnp.stack(forces, axis=3)
    return void_flat.reshape(NX, NY, NZ), drag
```

```python
import functools

import jax
import jax.numpy as jnp
from jax import lax
from jax.experimental import pallas as pl
from jax.experimental.pallas import tpu as pltpu
from jax.sharding import PartitionSpec as P

exponent = -2.65
drag_scale = 2.0
void_floor = 0.1

MESH = pl.DeviceIdType.MESH
DIRECTIONS = [(-1, 0), (1, 0), (0, -1), (0, 1), (-1, -1), (-1, 1), (1, -1), (1, 1)]


def rounded_up(count, unit):
    return (count + unit - 1) // unit * unit


def halves(value):
    high = value.astype(jnp.bfloat16)
    low = (value - high.astype(jnp.float32)).astype(jnp.bfloat16)
    return high, low


def kernel(
    sizes,
    live_ref,
    fluid_ref,
    velocity_ref,
    volume_ref,
    cells_ref,
    void_ref,
    drag_ref,
    spots,
    tile,
    wide,
    fields,
    out_x,
    out_y,
    out_c,
    in_x,
    in_y,
    in_c,
    flow_out_y,
    flow_out_c,
    flow_in_x,
    flow_in_y,
    flow_in_c,
    send_sem,
    recv_sem,
):
    count_x, count_y, cells_x, cells_y, pair, point_count = sizes
    wide_x, wide_y = cells_x + 2, cells_y + 2
    lanes = cells_ref.shape[-1]
    depth = tile.shape[1]
    rows = tile.shape[0]
    block_count = cells_ref.shape[0]
    turns = block_count // pair
    here_x, here_y = lax.axis_index("gx"), lax.axis_index("gy")

    def neighbour(direction):
        dx, dy = direction
        return (
            lax.rem(here_x + (dx + count_x), count_x),
            lax.rem(here_y + (dy + count_y), count_y),
        )

    barrier = pltpu.get_barrier_semaphore()
    for direction in DIRECTIONS:
        pl.semaphore_signal(barrier, inc=1, device_id=neighbour(direction), device_id_type=MESH)

    for side, j in enumerate((0, cells_y - 1)):
        for k in range(3):
            for i in range(cells_x):
                flow_out_y[side, k * cells_x + i : k * cells_x + i + 1] = fluid_ref[k, i, j : j + 1]
            for side_x, i in enumerate((0, cells_x - 1)):
                flow_out_c[side_x * 2 + side, k : k + 1] = fluid_ref[k, i, j : j + 1]

    alive_below = live_ref[0, 0]

    def shares(turn):
        parts = []
        for h in range(pair):
            block = turn * pair + h
            alive = jnp.where(
                jnp.full((1, lanes), block, jnp.int32) < alive_below, 1.0, 0.0
            )
            parts.append(volume_ref[pl.ds(block, 1), :] * alive / point_count)
        return jnp.concatenate(parts, axis=1)

    def cell_rows(turn, s):
        return jnp.concatenate(
            [cells_ref[turn * pair + h, s : s + 1, :] for h in range(pair)], axis=1
        )

    width = pair * lanes
    row_ids = lax.broadcasted_iota(jnp.int32, (rows, width), 0)
    depth_ids = lax.broadcasted_iota(jnp.int32, (depth, width), 0)

    def deposit(turn, total):
        high, low = halves(shares(turn))
        high, low = high.astype(jnp.float32), low.astype(jnp.float32)
        for s in range(point_count):
            cells = cell_rows(turn, s)
            spot = jnp.where(depth_ids == cells % depth, 1.0, 0.0).astype(jnp.bfloat16)
            spots[turn, s] = spot
            hit = row_ids == cells // depth
            weights = jnp.concatenate(
                [
                    jnp.where(hit, high, 0.0).astype(jnp.bfloat16),
                    jnp.where(hit, low, 0.0).astype(jnp.bfloat16),
                ],
                axis=0,
            )
            total = total + lax.dot_general(
                weights, spot, (((1,), (1,)), ((), ())), preferred_element_type=jnp.float32
            )
        return total

    total = jnp.zeros((2 * rows, depth), jnp.float32)
    first = turns // 2
    total = lax.fori_loop(0, first, deposit, total)

    pl.semaphore_wait(barrier, len(DIRECTIONS))

    def flow_copy(slot):
        dx, dy = DIRECTIONS[slot]
        side_x, side_y = int(dx > 0), int(dy > 0)
        if dy == 0:
            source, target = fluid_ref.at[:, side_x * (cells_x - 1)], flow_in_x.at[side_x]
        elif dx == 0:
            source, target = flow_out_y.at[side_y], flow_in_y.at[side_y]
        else:
            corner = side_x * 2 + side_y
            source, target = flow_out_c.at[corner], flow_in_c.at[corner]
        return pltpu.make_async_remote_copy(
            src_ref=source,
            dst_ref=target,
            send_sem=send_sem.at[8 + slot],
            recv_sem=recv_sem.at[8 + slot],
            device_id=neighbour(DIRECTIONS[slot]),
            device_id_type=MESH,
        )

    def volume_copy(slot):
        dx, dy = DIRECTIONS[slot]
        side_x, side_y = int(dx > 0), int(dy > 0)
        if dy == 0:
            source, target = out_x.at[side_x], in_x.at[side_x]
        elif dx == 0:
            source, target = out_y.at[side_y], in_y.at[side_y]
        else:
            corner = side_x * 2 + side_y
            source, target = out_c.at[corner], in_c.at[corner]
        return pltpu.make_async_remote_copy(
            src_ref=source,
            dst_ref=target,
            send_sem=send_sem.at[slot],
            recv_sem=recv_sem.at[slot],
            device_id=neighbour(DIRECTIONS[slot]),
            device_id_type=MESH,
        )

    for slot in range(8):
        flow_copy(slot).start()

    total = lax.fori_loop(first, turns, deposit, total)
    tile[...] = total[:rows] + total[rows:]

    band = 2 * wide_y
    top = (wide_x - 2) * wide_y
    out_x[0, :band] = tile[:band]
    out_x[1, :band] = tile[top : top + band]
    for side, j in enumerate((0, wide_y - 2)):
        for i in range(wide_x):
            out_y[side, 2 * i : 2 * i + 2] = tile[i * wide_y + j : i * wide_y + j + 2]
        for side_x, first_i in enumerate((0, wide_x - 2)):
            for step in range(2):
                start = (first_i + step) * wide_y + j
                out_c[side_x * 2 + side, 2 * step : 2 * step + 2] = tile[start : start + 2]

    for k in range(3):
        for i in range(cells_x):
            start = (i + 1) * wide_y + 1
            wide[k, start : start + cells_y] = fluid_ref[k, i]

    for slot in (4, 5, 6, 7, 0, 1, 2, 3):
        volume_copy(slot).start()

    spare = rows - wide_x * wide_y
    for k in range(3):
        if spare:
            wide[k, wide_x * wide_y :] = jnp.zeros((spare, depth), jnp.float32)
    for slot in range(8):
        flow_copy(slot).wait()
    for k in range(3):
        for side in range(2):
            i = wide_x - 1 if side == 0 else 0
            wide[k, i * wide_y + 1 : i * wide_y + 1 + cells_y] = flow_in_x[side, k]
            j = wide_y - 1 if side == 0 else 0
            for layer in range(cells_x):
                at = (layer + 1) * wide_y + j
                wide[k, at : at + 1] = flow_in_y[side, k * cells_x + layer : k * cells_x + layer + 1]
            for side_y in range(2):
                at = i * wide_y + (wide_y - 1 if side_y == 0 else 0)
                wide[k, at : at + 1] = flow_in_c[side * 2 + side_y, k : k + 1]

    for slot in range(8):
        volume_copy(slot).wait()
    tile[top : top + band] += in_x[0, :band]
    tile[:band] += in_x[1, :band]
    for side in range(2):
        j = wide_y - 2 if side == 0 else 0
        for i in range(wide_x):
            tile[i * wide_y + j : i * wide_y + j + 2] += in_y[side, 2 * i : 2 * i + 2]
        for side_x in range(2):
            first_i = wide_x - 2 if side_x == 0 else 0
            for step in range(2):
                start = (first_i + step) * wide_y + j
                tile[start : start + 2] += in_c[side_x * 2 + side, 2 * step : 2 * step + 2]

    void = jnp.maximum(1.0 - tile[...], void_floor)
    tile[...] = void
    resistance = jnp.exp(exponent * jnp.log(void))
    for k in range(4):
        high, low = halves(resistance * wide[k] if k < 3 else resistance)
        fields[k * rows : (k + 1) * rows, :depth] = high
        fields[k * rows : (k + 1) * rows, depth:] = low
    for i in range(cells_x):
        start = (i + 1) * wide_y + 1
        void_ref[i] = tile[start : start + cells_y]

    def pull(turn, carry):
        sums = [jnp.zeros((8, width), jnp.float32) for _ in range(4)]
        for s in range(point_count):
            spot = spots[turn, s]
            picked = jnp.dot(
                fields[...],
                jnp.concatenate([spot, spot], axis=0),
                preferred_element_type=jnp.float32,
            )
            hit = row_ids == cell_rows(turn, s) // depth
            for k in range(4):
                chosen = jnp.where(hit, picked[k * rows : (k + 1) * rows], 0.0)
                sums[k] = sums[k] + jnp.sum(chosen.reshape(rows // 8, 8, width), axis=0)
        share = shares(turn)
        weight_sum = jnp.sum(sums[3], axis=0, keepdims=True)
        for k in range(3):
            pulling = jnp.sum(sums[k], axis=0, keepdims=True)
            for h in range(pair):
                at = slice(h * lanes, (h + 1) * lanes)
                block = turn * pair + h
                drag_ref[block, k : k + 1] = (
                    drag_scale
                    * share[:, at]
                    * (pulling[:, at] - velocity_ref[block, k : k + 1] * weight_sum[:, at])
                )
        return carry

    lax.fori_loop(0, turns, pull, 0)


def body(fluid_velocity, particle_velocity, particle_volume, satellite_cells, live_blocks):
    _, cells_x, cells_y, depth = fluid_velocity.shape
    wide_x, wide_y = cells_x + 2, cells_y + 2
    satellites = satellite_cells[0, 0]
    block_count, point_count, lanes = satellites.shape
    pair = 2 if block_count % 2 == 0 else 1
    rows = rounded_up(wide_x * wide_y, 16)
    band = rounded_up(2 * wide_y, 8)
    sides = rounded_up(2 * wide_x, 8)
    flow_sides = rounded_up(3 * cells_x, 8)
    sizes = (lax.axis_size("gx"), lax.axis_size("gy"), cells_x, cells_y, pair, point_count)
    vmem = pl.BlockSpec(memory_space=pltpu.VMEM)
    f32 = jnp.float32
    void_fraction, drag = pl.pallas_call(
        functools.partial(kernel, sizes),
        out_shape=(
            jax.ShapeDtypeStruct((cells_x, cells_y, depth), f32),
            jax.ShapeDtypeStruct((block_count, 3, lanes), f32),
        ),
        in_specs=[pl.BlockSpec(memory_space=pltpu.SMEM), vmem, vmem, vmem, vmem],
        out_specs=(vmem, vmem),
        scratch_shapes=[
            pltpu.VMEM((block_count // pair, point_count, depth, pair * lanes), jnp.bfloat16),
            pltpu.VMEM((rows, depth), f32),
            pltpu.VMEM((3, rows, depth), f32),
            pltpu.VMEM((4 * rows, 2 * depth), jnp.bfloat16),
            pltpu.VMEM((2, band, depth), f32),
            pltpu.VMEM((2, sides, depth), f32),
            pltpu.VMEM((4, 8, depth), f32),
            pltpu.VMEM((2, band, depth), f32),
            pltpu.VMEM((2, sides, depth), f32),
            pltpu.VMEM((4, 8, depth), f32),
            pltpu.VMEM((2, flow_sides, depth), f32),
            pltpu.VMEM((4, 8, depth), f32),
            pltpu.VMEM((2, 3, cells_y, depth), f32),
            pltpu.VMEM((2, flow_sides, depth), f32),
            pltpu.VMEM((4, 8, depth), f32),
            pltpu.SemaphoreType.DMA((16,)),
            pltpu.SemaphoreType.DMA((16,)),
        ],
        compiler_params=pltpu.CompilerParams(collective_id=0, has_side_effects=True),
    )(live_blocks, fluid_velocity, particle_velocity[0, 0], particle_volume[0, 0], satellites)
    return void_fraction, drag[None, None]


def solution(mesh):
    placed = (
        P(None, "gx", "gy", None),
        P("gx", "gy", None, None, None),
        P("gx", "gy", None, None),
        P("gx", "gy", None, None, None),
        P("gx", "gy"),
    )
    return jax.shard_map(
        body,
        mesh=mesh,
        in_specs=placed,
        out_specs=(P("gx", "gy", None), P("gx", "gy", None, None, None)),
        check_vma=False,
    )
```

```python
import functools

import jax
import jax.numpy as jnp
from jax import lax
from jax.experimental import pallas as pl
from jax.experimental.pallas import tpu as pltpu
from jax.sharding import PartitionSpec as P

exponent = -2.65
drag_scale = 2.0
void_floor = 0.1

MESH = pl.DeviceIdType.MESH
DIRECTIONS = [(-1, 0), (1, 0), (0, -1), (0, 1), (-1, -1), (-1, 1), (1, -1), (1, 1)]


def rounded_up(count, unit):
    return (count + unit - 1) // unit * unit


def halves(value):
    high = value.astype(jnp.bfloat16)
    low = (value - high.astype(jnp.float32)).astype(jnp.bfloat16)
    return high, low


def kernel(
    sizes,
    live_ref,
    fluid_ref,
    velocity_ref,
    volume_ref,
    cells_ref,
    void_ref,
    drag_ref,
    spots,
    tile,
    wide,
    fields,
    out_x,
    out_y,
    out_c,
    in_x,
    in_y,
    in_c,
    flow_out_y,
    flow_out_c,
    flow_in_x,
    flow_in_y,
    flow_in_c,
    send_sem,
    recv_sem,
):
    count_x, count_y, cells_x, cells_y, pair, point_count = sizes
    wide_x, wide_y = cells_x + 2, cells_y + 2
    lanes = cells_ref.shape[-1]
    depth = tile.shape[1]
    rows = tile.shape[0]
    block_count = cells_ref.shape[1]
    turns = block_count // pair
    here_x, here_y = lax.axis_index("gx"), lax.axis_index("gy")

    def neighbour(direction):
        dx, dy = direction
        return (
            lax.rem(here_x + (dx + count_x), count_x),
            lax.rem(here_y + (dy + count_y), count_y),
        )

    barrier = pltpu.get_barrier_semaphore()
    for direction in DIRECTIONS:
        pl.semaphore_signal(barrier, inc=1, device_id=neighbour(direction), device_id_type=MESH)

    for side, j in enumerate((0, cells_y - 1)):
        for k in range(3):
            for i in range(cells_x):
                flow_out_y[side, k * cells_x + i : k * cells_x + i + 1] = fluid_ref[k, i, j : j + 1]
            for side_x, i in enumerate((0, cells_x - 1)):
                flow_out_c[side_x * 2 + side, k : k + 1] = fluid_ref[k, i, j : j + 1]

    alive_below = jnp.broadcast_to(live_ref[...], (1, lanes))
    half = rows // 2
    width = pair * lanes

    def shares(turn):
        parts = []
        for h in range(pair):
            block = turn * pair + h
            alive = jnp.where(alive_below > block, 1.0, 0.0)
            parts.append(volume_ref[block : block + 1, :] * alive / point_count)
        return jnp.concatenate(parts, axis=1)

    def cell_rows(turn, s):
        return jnp.concatenate(
            [cells_ref[s, turn * pair + h : turn * pair + h + 1, :] for h in range(pair)], axis=1
        )

    def narrow_rows(row, count):
        tall = jnp.broadcast_to(row.astype(jnp.float32), (16, width)).astype(jnp.bfloat16)
        return jnp.concatenate([tall] * (count // 16), axis=0)

    def narrow_ids(count):
        return lax.broadcasted_iota(jnp.int32, (count, width), 0).astype(jnp.float32)

    place_ids = narrow_ids(2 * depth).astype(jnp.bfloat16)
    both_ids = jnp.concatenate([narrow_ids(half)] * 2, axis=0).astype(jnp.bfloat16)
    one = jnp.ones((), jnp.bfloat16)
    zero = jnp.zeros((), jnp.bfloat16)

    def deposit(turn, totals):
        high, low = halves(shares(turn))
        split = jnp.concatenate(
            [
                jnp.broadcast_to(high.astype(jnp.float32), (half, width)),
                jnp.broadcast_to(low.astype(jnp.float32), (half, width)),
            ],
            axis=0,
        ).astype(jnp.bfloat16)
        totals = list(totals)
        for s in range(point_count):
            cells = cell_rows(turn, s)
            spot = jnp.where(place_ids == narrow_rows(cells % (2 * depth), 2 * depth), one, zero)
            spots[turn, s] = spot
            weights = jnp.where(
                both_ids == narrow_rows(cells // (2 * depth), 2 * half), split, zero
            )
            totals[s % 2] = totals[s % 2] + lax.dot_general(
                weights, spot, (((1,), (1,)), ((), ())), preferred_element_type=jnp.float32
            )
        return totals

    totals = [jnp.zeros((2 * half, 2 * depth), jnp.float32)] * 2
    first = turns // 2
    for turn in range(first):
        totals = deposit(turn, totals)

    pl.semaphore_wait(barrier, len(DIRECTIONS))

    def flow_copy(slot):
        dx, dy = DIRECTIONS[slot]
        side_x, side_y = int(dx > 0), int(dy > 0)
        if dy == 0:
            source, target = fluid_ref.at[:, side_x * (cells_x - 1)], flow_in_x.at[side_x]
        elif dx == 0:
            source, target = flow_out_y.at[side_y], flow_in_y.at[side_y]
        else:
            corner = side_x * 2 + side_y
            source, target = flow_out_c.at[corner], flow_in_c.at[corner]
        return pltpu.make_async_remote_copy(
            src_ref=source,
            dst_ref=target,
            send_sem=send_sem.at[8 + slot],
            recv_sem=recv_sem.at[8 + slot],
            device_id=neighbour(DIRECTIONS[slot]),
            device_id_type=MESH,
        )

    def volume_copy(slot):
        dx, dy = DIRECTIONS[slot]
        side_x, side_y = int(dx > 0), int(dy > 0)
        if dy == 0:
            source, target = out_x.at[side_x], in_x.at[side_x]
        elif dx == 0:
            source, target = out_y.at[side_y], in_y.at[side_y]
        else:
            corner = side_x * 2 + side_y
            source, target = out_c.at[corner], in_c.at[corner]
        return pltpu.make_async_remote_copy(
            src_ref=source,
            dst_ref=target,
            send_sem=send_sem.at[slot],
            recv_sem=recv_sem.at[slot],
            device_id=neighbour(DIRECTIONS[slot]),
            device_id_type=MESH,
        )

    for slot in range(8):
        flow_copy(slot).start()

    for turn in range(first, turns):
        totals = deposit(turn, totals)
    total = totals[0] + totals[1]
    total = total[:half] + total[half:]
    evens, odds = pl.ds(0, half, stride=2), pl.ds(1, half, stride=2)
    tile[evens] = total[:, :depth]
    tile[odds] = total[:, depth:]

    band = 2 * wide_y
    top = (wide_x - 2) * wide_y
    out_x[0, :band] = tile[:band]
    out_x[1, :band] = tile[top : top + band]
    for side, j in enumerate((0, wide_y - 2)):
        for i in range(wide_x):
            out_y[side, 2 * i : 2 * i + 2] = tile[i * wide_y + j : i * wide_y + j + 2]
        for side_x, first_i in enumerate((0, wide_x - 2)):
            for step in range(2):
                start = (first_i + step) * wide_y + j
                out_c[side_x * 2 + side, 2 * step : 2 * step + 2] = tile[start : start + 2]

    for k in range(3):
        for i in range(cells_x):
            start = (i + 1) * wide_y + 1
            wide[k, start : start + cells_y] = fluid_ref[k, i]

    for slot in (4, 5, 6, 7, 0, 1, 2, 3):
        volume_copy(slot).start()

    spare = rows - wide_x * wide_y
    for k in range(3):
        if spare:
            wide[k, wide_x * wide_y :] = jnp.zeros((spare, depth), jnp.float32)
    for slot in range(8):
        flow_copy(slot).wait()
    for k in range(3):
        for side in range(2):
            i = wide_x - 1 if side == 0 else 0
            wide[k, i * wide_y + 1 : i * wide_y + 1 + cells_y] = flow_in_x[side, k]
            j = wide_y - 1 if side == 0 else 0
            for layer in range(cells_x):
                at = (layer + 1) * wide_y + j
                wide[k, at : at + 1] = flow_in_y[side, k * cells_x + layer : k * cells_x + layer + 1]
            for side_y in range(2):
                at = i * wide_y + (wide_y - 1 if side_y == 0 else 0)
                wide[k, at : at + 1] = flow_in_c[side * 2 + side_y, k : k + 1]

    for slot in range(8):
        volume_copy(slot).wait()
    tile[top : top + band] += in_x[0, :band]
    tile[:band] += in_x[1, :band]
    for side in range(2):
        j = wide_y - 2 if side == 0 else 0
        for i in range(wide_x):
            tile[i * wide_y + j : i * wide_y + j + 2] += in_y[side, 2 * i : 2 * i + 2]
        for side_x in range(2):
            first_i = wide_x - 2 if side_x == 0 else 0
            for step in range(2):
                start = (first_i + step) * wide_y + j
                tile[start : start + 2] += in_c[side_x * 2 + side, 2 * step : 2 * step + 2]

    void = jnp.maximum(1.0 - tile[...], void_floor)
    tile[...] = void
    void = jnp.concatenate([tile[evens], tile[odds]], axis=1)
    resistance = jnp.exp(exponent * jnp.log(void))
    parts = [
        resistance * jnp.concatenate([wide[k, evens], wide[k, odds]], axis=1) for k in range(3)
    ] + [resistance]
    mixed = jnp.concatenate(
        [part[g * 8 : (g + 1) * 8] for g in range(half // 8) for part in parts], axis=0
    )
    high, low = halves(mixed)
    fields[:, : 2 * depth] = high
    fields[:, 2 * depth :] = low
    for i in range(cells_x):
        start = (i + 1) * wide_y + 1
        void_ref[i] = tile[start : start + cells_y]

    group_ids = lax.broadcasted_iota(jnp.int32, (8, width), 0)
    for turn in range(turns):
        sums = [jnp.zeros((8, width), jnp.float32) for _ in range(4)]
        for s in range(point_count):
            spot = spots[turn, s]
            picked = jnp.dot(
                fields[...],
                jnp.concatenate([spot, spot], axis=0),
                preferred_element_type=jnp.float32,
            )
            row = jnp.broadcast_to(cell_rows(turn, s) // (2 * depth), (8, width))
            for g in range(half // 8):
                hit = row == group_ids + 8 * g
                for k in range(4):
                    at = (g * 4 + k) * 8
                    sums[k] = sums[k] + jnp.where(hit, picked[at : at + 8], 0.0)
        share = shares(turn)
        weight_sum = jnp.sum(sums[3], axis=0, keepdims=True)
        for k in range(3):
            pulling = jnp.sum(sums[k], axis=0, keepdims=True)
            for h in range(pair):
                at = slice(h * lanes, (h + 1) * lanes)
                block = turn * pair + h
                drag_ref[k, block : block + 1] = (
                    drag_scale
                    * share[:, at]
                    * (pulling[:, at] - velocity_ref[k, block : block + 1] * weight_sum[:, at])
                )


def body(fluid_velocity, particle_velocity, particle_volume, satellite_cells, live_blocks):
    _, cells_x, cells_y, depth = fluid_velocity.shape
    wide_x, wide_y = cells_x + 2, cells_y + 2
    satellites = satellite_cells[0, 0]
    block_count, point_count, lanes = satellites.shape
    pair = 2 if block_count % 2 == 0 else 1
    rows = rounded_up(wide_x * wide_y, 16)
    band = rounded_up(2 * wide_y, 8)
    sides = rounded_up(2 * wide_x, 8)
    flow_sides = rounded_up(3 * cells_x, 8)
    sizes = (lax.axis_size("gx"), lax.axis_size("gy"), cells_x, cells_y, pair, point_count)
    vmem = pl.BlockSpec(memory_space=pltpu.VMEM)
    f32 = jnp.float32
    void_fraction, drag = pl.pallas_call(
        functools.partial(kernel, sizes),
        out_shape=(
            jax.ShapeDtypeStruct((cells_x, cells_y, depth), f32),
            jax.ShapeDtypeStruct((3, block_count, lanes), f32),
        ),
        in_specs=[vmem] * 5,
        out_specs=(vmem, vmem),
        scratch_shapes=[
            pltpu.VMEM((block_count // pair, point_count, 2 * depth, pair * lanes), jnp.bfloat16),
            pltpu.VMEM((rows, depth), f32),
            pltpu.VMEM((3, rows, depth), f32),
            pltpu.VMEM((2 * rows, 4 * depth), jnp.bfloat16),
            pltpu.VMEM((2, band, depth), f32),
            pltpu.VMEM((2, sides, depth), f32),
            pltpu.VMEM((4, 8, depth), f32),
            pltpu.VMEM((2, band, depth), f32),
            pltpu.VMEM((2, sides, depth), f32),
            pltpu.VMEM((4, 8, depth), f32),
            pltpu.VMEM((2, flow_sides, depth), f32),
            pltpu.VMEM((4, 8, depth), f32),
            pltpu.VMEM((2, 3, cells_y, depth), f32),
            pltpu.VMEM((2, flow_sides, depth), f32),
            pltpu.VMEM((4, 8, depth), f32),
            pltpu.SemaphoreType.DMA((16,)),
            pltpu.SemaphoreType.DMA((16,)),
        ],
        compiler_params=pltpu.CompilerParams(collective_id=0, has_side_effects=True),
    )(
        live_blocks,
        fluid_velocity,
        jnp.swapaxes(particle_velocity[0, 0], 0, 1),
        particle_volume[0, 0],
        jnp.swapaxes(satellites, 0, 1),
    )
    return void_fraction, jnp.swapaxes(drag, 0, 1)[None, None]


def solution(mesh):
    placed = (
        P(None, "gx", "gy", None),
        P("gx", "gy", None, None, None),
        P("gx", "gy", None, None),
        P("gx", "gy", None, None, None),
        P("gx", "gy"),
    )
    return jax.shard_map(
        body,
        mesh=mesh,
        in_specs=placed,
        out_specs=(P("gx", "gy", None), P("gx", "gy", None, None, None)),
        check_vma=False,
    )
```

```python
import functools

import jax
import jax.numpy as jnp
from jax import lax
from jax.experimental import pallas as pl
from jax.experimental.pallas import tpu as pltpu
from jax.sharding import PartitionSpec as P

exponent = -2.65
drag_scale = 2.0
void_floor = 0.1

MESH = pl.DeviceIdType.MESH
DIRECTIONS = [(-1, 0), (1, 0), (0, -1), (0, 1), (-1, -1), (-1, 1), (1, -1), (1, 1)]


def rounded_up(count, unit):
    return (count + unit - 1) // unit * unit


def halves(value):
    high = value.astype(jnp.bfloat16)
    low = (value - high.astype(jnp.float32)).astype(jnp.bfloat16)
    return high, low


def kernel(
    sizes,
    live_ref,
    fluid_hbm,
    velocity_hbm,
    volume_hbm,
    cells_hbm,
    void_ref,
    drag_ref,
    fluid_ref,
    velocity_ref,
    volume_ref,
    cells_ref,
    load_sem,
    spots,
    tile,
    wide,
    fields,
    out_x,
    out_y,
    out_c,
    in_x,
    in_y,
    in_c,
    flow_out_y,
    flow_out_c,
    flow_in_x,
    flow_in_y,
    flow_in_c,
    send_sem,
    recv_sem,
):
    count_x, count_y, cells_x, cells_y, pair, point_count = sizes
    wide_x, wide_y = cells_x + 2, cells_y + 2
    lanes = cells_ref.shape[-1]
    depth = tile.shape[1]
    rows = tile.shape[0]
    block_count = cells_ref.shape[1]
    turns = block_count // pair
    here_x, here_y = lax.axis_index("gx"), lax.axis_index("gy")

    def neighbour(direction):
        dx, dy = direction
        return (
            lax.rem(here_x + (dx + count_x), count_x),
            lax.rem(here_y + (dy + count_y), count_y),
        )

    loads = [
        pltpu.make_async_copy(source, target, load_sem.at[at])
        for at, (source, target) in enumerate(
            (
                (cells_hbm, cells_ref),
                (volume_hbm, volume_ref),
                (fluid_hbm, fluid_ref),
                (velocity_hbm, velocity_ref),
            )
        )
    ]
    for load in loads:
        load.start()
    barrier = pltpu.get_barrier_semaphore()
    for direction in DIRECTIONS:
        pl.semaphore_signal(barrier, inc=1, device_id=neighbour(direction), device_id_type=MESH)

    loads[0].wait()
    loads[1].wait()
    alive_below = jnp.broadcast_to(live_ref[...], (1, lanes))
    half = rows // 2
    width = pair * lanes

    def shares(turn):
        parts = []
        for h in range(pair):
            block = turn * pair + h
            alive = jnp.where(alive_below > block, 1.0, 0.0)
            parts.append(volume_ref[block : block + 1, :] * alive / point_count)
        return jnp.concatenate(parts, axis=1)

    def cell_rows(turn, s):
        return jnp.concatenate(
            [cells_ref[s, turn * pair + h : turn * pair + h + 1, :] for h in range(pair)], axis=1
        )

    def narrow_rows(row, count):
        tall = jnp.broadcast_to(row.astype(jnp.float32), (16, width)).astype(jnp.bfloat16)
        return jnp.concatenate([tall] * (count // 16), axis=0)

    def narrow_ids(count):
        return lax.broadcasted_iota(jnp.int32, (count, width), 0).astype(jnp.float32)

    place_ids = narrow_ids(2 * depth).astype(jnp.bfloat16)
    both_ids = jnp.concatenate([narrow_ids(half)] * 2, axis=0).astype(jnp.bfloat16)
    one = jnp.ones((), jnp.bfloat16)
    zero = jnp.zeros((), jnp.bfloat16)

    def deposit(turn, totals):
        high, low = halves(shares(turn))
        split = jnp.concatenate(
            [
                jnp.broadcast_to(high.astype(jnp.float32), (half, width)),
                jnp.broadcast_to(low.astype(jnp.float32), (half, width)),
            ],
            axis=0,
        ).astype(jnp.bfloat16)
        totals = list(totals)
        for s in range(point_count):
            cells = cell_rows(turn, s)
            spot = jnp.where(place_ids == narrow_rows(cells % (2 * depth), 2 * depth), one, zero)
            spots[turn, s] = spot
            weights = jnp.where(
                both_ids == narrow_rows(cells // (2 * depth), 2 * half), split, zero
            )
            for p in range(2):
                totals[p] = totals[p] + lax.dot_general(
                    weights,
                    spot[p * depth : (p + 1) * depth],
                    (((1,), (1,)), ((), ())),
                    preferred_element_type=jnp.float32,
                )
        return totals

    totals = [jnp.zeros((2 * half, depth), jnp.float32)] * 2
    first = turns // 2
    for turn in range(first):
        totals = deposit(turn, totals)

    loads[2].wait()
    loads[3].wait()
    for side, j in enumerate((0, cells_y - 1)):
        for k in range(3):
            for i in range(cells_x):
                flow_out_y[side, k * cells_x + i : k * cells_x + i + 1] = fluid_ref[k, i, j : j + 1]
            for side_x, i in enumerate((0, cells_x - 1)):
                flow_out_c[side_x * 2 + side, k : k + 1] = fluid_ref[k, i, j : j + 1]

    pl.semaphore_wait(barrier, len(DIRECTIONS))

    def flow_copy(slot):
        dx, dy = DIRECTIONS[slot]
        side_x, side_y = int(dx > 0), int(dy > 0)
        if dy == 0:
            source, target = fluid_ref.at[:, side_x * (cells_x - 1)], flow_in_x.at[side_x]
        elif dx == 0:
            source, target = flow_out_y.at[side_y], flow_in_y.at[side_y]
        else:
            corner = side_x * 2 + side_y
            source, target = flow_out_c.at[corner], flow_in_c.at[corner]
        return pltpu.make_async_remote_copy(
            src_ref=source,
            dst_ref=target,
            send_sem=send_sem.at[8 + slot],
            recv_sem=recv_sem.at[8 + slot],
            device_id=neighbour(DIRECTIONS[slot]),
            device_id_type=MESH,
        )

    def volume_copy(slot):
        dx, dy = DIRECTIONS[slot]
        side_x, side_y = int(dx > 0), int(dy > 0)
        if dy == 0:
            source, target = out_x.at[side_x], in_x.at[side_x]
        elif dx == 0:
            source, target = out_y.at[side_y], in_y.at[side_y]
        else:
            corner = side_x * 2 + side_y
            source, target = out_c.at[corner], in_c.at[corner]
        return pltpu.make_async_remote_copy(
            src_ref=source,
            dst_ref=target,
            send_sem=send_sem.at[slot],
            recv_sem=recv_sem.at[slot],
            device_id=neighbour(DIRECTIONS[slot]),
            device_id_type=MESH,
        )

    for slot in range(8):
        flow_copy(slot).start()

    for turn in range(first, turns):
        totals = deposit(turn, totals)
    evens, odds = pl.ds(0, half, stride=2), pl.ds(1, half, stride=2)
    tile[evens] = totals[0][:half] + totals[0][half:]
    tile[odds] = totals[1][:half] + totals[1][half:]

    band = 2 * wide_y
    top = (wide_x - 2) * wide_y
    out_x[0, :band] = tile[:band]
    out_x[1, :band] = tile[top : top + band]
    for side, j in enumerate((0, wide_y - 2)):
        for i in range(wide_x):
            out_y[side, 2 * i : 2 * i + 2] = tile[i * wide_y + j : i * wide_y + j + 2]
        for side_x, first_i in enumerate((0, wide_x - 2)):
            for step in range(2):
                start = (first_i + step) * wide_y + j
                out_c[side_x * 2 + side, 2 * step : 2 * step + 2] = tile[start : start + 2]

    for k in range(3):
        for i in range(cells_x):
            start = (i + 1) * wide_y + 1
            wide[k, start : start + cells_y] = fluid_ref[k, i]

    for slot in (4, 5, 6, 7, 0, 1, 2, 3):
        volume_copy(slot).start()

    spare = rows - wide_x * wide_y
    for k in range(3):
        if spare:
            wide[k, wide_x * wide_y :] = jnp.zeros((spare, depth), jnp.float32)
    for slot in range(8):
        flow_copy(slot).wait()
    for k in range(3):
        for side in range(2):
            i = wide_x - 1 if side == 0 else 0
            wide[k, i * wide_y + 1 : i * wide_y + 1 + cells_y] = flow_in_x[side, k]
            j = wide_y - 1 if side == 0 else 0
            for layer in range(cells_x):
                at = (layer + 1) * wide_y + j
                wide[k, at : at + 1] = flow_in_y[side, k * cells_x + layer : k * cells_x + layer + 1]
            for side_y in range(2):
                at = i * wide_y + (wide_y - 1 if side_y == 0 else 0)
                wide[k, at : at + 1] = flow_in_c[side * 2 + side_y, k : k + 1]

    for slot in range(8):
        volume_copy(slot).wait()
    tile[top : top + band] += in_x[0, :band]
    tile[:band] += in_x[1, :band]
    for side in range(2):
        j = wide_y - 2 if side == 0 else 0
        for i in range(wide_x):
            tile[i * wide_y + j : i * wide_y + j + 2] += in_y[side, 2 * i : 2 * i + 2]
        for side_x in range(2):
            first_i = wide_x - 2 if side_x == 0 else 0
            for step in range(2):
                start = (first_i + step) * wide_y + j
                tile[start : start + 2] += in_c[side_x * 2 + side, 2 * step : 2 * step + 2]

    void = jnp.maximum(1.0 - tile[...], void_floor)
    tile[...] = void
    void = jnp.concatenate([tile[evens], tile[odds]], axis=1)
    resistance = jnp.exp(exponent * jnp.log(void))
    parts = [
        resistance * jnp.concatenate([wide[k, evens], wide[k, odds]], axis=1) for k in range(3)
    ] + [resistance]
    mixed = jnp.concatenate(
        [part[g * 8 : (g + 1) * 8] for g in range(half // 8) for part in parts], axis=0
    )
    high, low = halves(mixed)
    fields[: 4 * half] = high
    fields[4 * half :] = low
    for i in range(cells_x):
        start = (i + 1) * wide_y + 1
        void_ref[i] = tile[start : start + cells_y]

    group_ids = lax.broadcasted_iota(jnp.int32, (8, width), 0)
    for turn in range(turns):
        sums = [jnp.zeros((8, width), jnp.float32) for _ in range(4)]
        for s in range(point_count):
            spot = spots[turn, s]
            picked = jnp.dot(fields[...], spot, preferred_element_type=jnp.float32)
            row = jnp.broadcast_to(cell_rows(turn, s) // (2 * depth), (8, width))
            for g in range(half // 8):
                hit = row == group_ids + 8 * g
                for k in range(4):
                    at = (g * 4 + k) * 8
                    value = picked[at : at + 8] + picked[4 * half + at : 4 * half + at + 8]
                    sums[k] = sums[k] + jnp.where(hit, value, 0.0)
        share = shares(turn)
        weight_sum = jnp.sum(sums[3], axis=0, keepdims=True)
        for k in range(3):
            pulling = jnp.sum(sums[k], axis=0, keepdims=True)
            for h in range(pair):
                at = slice(h * lanes, (h + 1) * lanes)
                block = turn * pair + h
                drag_ref[k, block : block + 1] = (
                    drag_scale
                    * share[:, at]
                    * (pulling[:, at] - velocity_ref[k, block : block + 1] * weight_sum[:, at])
                )


def body(fluid_velocity, particle_velocity, particle_volume, satellite_cells, live_blocks):
    _, cells_x, cells_y, depth = fluid_velocity.shape
    wide_x, wide_y = cells_x + 2, cells_y + 2
    satellites = satellite_cells[0, 0]
    block_count, point_count, lanes = satellites.shape
    pair = 2 if block_count % 2 == 0 else 1
    rows = rounded_up(wide_x * wide_y, 16)
    band = rounded_up(2 * wide_y, 8)
    sides = rounded_up(2 * wide_x, 8)
    flow_sides = rounded_up(3 * cells_x, 8)
    sizes = (lax.axis_size("gx"), lax.axis_size("gy"), cells_x, cells_y, pair, point_count)
    vmem = pl.BlockSpec(memory_space=pltpu.VMEM)
    f32 = jnp.float32
    void_fraction, drag = pl.pallas_call(
        functools.partial(kernel, sizes),
        out_shape=(
            jax.ShapeDtypeStruct((cells_x, cells_y, depth), f32),
            jax.ShapeDtypeStruct((3, block_count, lanes), f32),
        ),
        in_specs=[vmem] + [pl.BlockSpec(memory_space=pltpu.HBM)] * 4,
        out_specs=(vmem, vmem),
        scratch_shapes=[
            pltpu.VMEM(fluid_velocity.shape, f32),
            pltpu.VMEM((3, block_count, lanes), f32),
            pltpu.VMEM((block_count, lanes), f32),
            pltpu.VMEM((point_count, block_count, lanes), jnp.int32),
            pltpu.SemaphoreType.DMA((4,)),
            pltpu.VMEM((block_count // pair, point_count, 2 * depth, pair * lanes), jnp.bfloat16),
            pltpu.VMEM((rows, depth), f32),
            pltpu.VMEM((3, rows, depth), f32),
            pltpu.VMEM((4 * rows, 2 * depth), jnp.bfloat16),
            pltpu.VMEM((2, band, depth), f32),
            pltpu.VMEM((2, sides, depth), f32),
            pltpu.VMEM((4, 8, depth), f32),
            pltpu.VMEM((2, band, depth), f32),
            pltpu.VMEM((2, sides, depth), f32),
            pltpu.VMEM((4, 8, depth), f32),
            pltpu.VMEM((2, flow_sides, depth), f32),
            pltpu.VMEM((4, 8, depth), f32),
            pltpu.VMEM((2, 3, cells_y, depth), f32),
            pltpu.VMEM((2, flow_sides, depth), f32),
            pltpu.VMEM((4, 8, depth), f32),
            pltpu.SemaphoreType.DMA((16,)),
            pltpu.SemaphoreType.DMA((16,)),
        ],
        compiler_params=pltpu.CompilerParams(
            collective_id=0, has_side_effects=True, vmem_limit_bytes=16 * 1024 * 1024
        ),
    )(
        live_blocks,
        fluid_velocity,
        jnp.swapaxes(particle_velocity[0, 0], 0, 1),
        particle_volume[0, 0],
        jnp.swapaxes(satellites, 0, 1),
    )
    return void_fraction, jnp.swapaxes(drag, 0, 1)[None, None]


def solution(mesh):
    placed = (
        P(None, "gx", "gy", None),
        P("gx", "gy", None, None, None),
        P("gx", "gy", None, None),
        P("gx", "gy", None, None, None),
        P("gx", "gy"),
    )
    return jax.shard_map(
        body,
        mesh=mesh,
        in_specs=placed,
        out_specs=(P("gx", "gy", None), P("gx", "gy", None, None, None)),
        check_vma=False,
    )
```

```python
import functools

import jax
import jax.numpy as jnp
from jax import lax
from jax.experimental import pallas as pl
from jax.experimental.pallas import tpu as pltpu
from jax.sharding import PartitionSpec as P

exponent = -2.65
drag_scale = 2.0
void_floor = 0.1

MESH = pl.DeviceIdType.MESH
DIRECTIONS = [(-1, 0), (1, 0), (0, -1), (0, 1), (-1, -1), (-1, 1), (1, -1), (1, 1)]


def rounded_up(count, unit):
    return (count + unit - 1) // unit * unit


def halves(value):
    high = value.astype(jnp.bfloat16)
    low = (value - high.astype(jnp.float32)).astype(jnp.bfloat16)
    return high, low


def kernel(
    sizes,
    live_ref,
    fluid_hbm,
    velocity_hbm,
    volume_hbm,
    cells_hbm,
    void_ref,
    drag_ref,
    fluid_ref,
    velocity_ref,
    volume_ref,
    cells_ref,
    load_sem,
    spots,
    tile,
    wide,
    fields,
    out_x,
    out_y,
    out_c,
    in_x,
    in_y,
    in_c,
    flow_out_y,
    flow_out_c,
    flow_in_x,
    flow_in_y,
    flow_in_c,
    send_sem,
    recv_sem,
):
    count_x, count_y, cells_x, cells_y, pair, point_count = sizes
    wide_x, wide_y = cells_x + 2, cells_y + 2
    lanes = cells_ref.shape[-1]
    depth = tile.shape[1]
    rows = tile.shape[0]
    block_count = cells_ref.shape[1]
    turns = block_count // pair
    here_x, here_y = lax.axis_index("gx"), lax.axis_index("gy")

    def neighbour(direction):
        dx, dy = direction
        return (
            lax.rem(here_x + (dx + count_x), count_x),
            lax.rem(here_y + (dy + count_y), count_y),
        )

    loads = [
        pltpu.make_async_copy(source, target, load_sem.at[at])
        for at, (source, target) in enumerate(
            (
                (cells_hbm, cells_ref),
                (volume_hbm, volume_ref),
                (fluid_hbm, fluid_ref),
                (velocity_hbm, velocity_ref),
            )
        )
    ]
    for load in loads:
        load.start()
    barrier = pltpu.get_barrier_semaphore()
    for direction in DIRECTIONS:
        pl.semaphore_signal(barrier, inc=1, device_id=neighbour(direction), device_id_type=MESH)

    loads[0].wait()
    loads[1].wait()
    alive_below = jnp.broadcast_to(live_ref[...], (1, lanes))
    half = rows // 2
    width = pair * lanes

    def shares(turn):
        parts = []
        for h in range(pair):
            block = turn * pair + h
            alive = jnp.where(alive_below > block, 1.0, 0.0)
            parts.append(volume_ref[block : block + 1, :] * alive / point_count)
        return jnp.concatenate(parts, axis=1)

    def cell_rows(turn, s):
        return jnp.concatenate(
            [cells_ref[s, turn * pair + h : turn * pair + h + 1, :] for h in range(pair)], axis=1
        )

    def narrow_rows(row, count):
        tall = jnp.broadcast_to(row.astype(jnp.float32), (16, width)).astype(jnp.bfloat16)
        return jnp.concatenate([tall] * (count // 16), axis=0)

    def narrow_ids(count):
        return lax.broadcasted_iota(jnp.int32, (count, width), 0).astype(jnp.float32)

    place_ids = narrow_ids(2 * depth).astype(jnp.bfloat16)
    both_ids = jnp.concatenate([narrow_ids(half)] * 2, axis=0).astype(jnp.bfloat16)
    one = jnp.ones((), jnp.bfloat16)
    zero = jnp.zeros((), jnp.bfloat16)

    def deposit(turn, totals):
        high, low = halves(shares(turn))
        split = jnp.concatenate(
            [
                jnp.broadcast_to(high.astype(jnp.float32), (half, width)),
                jnp.broadcast_to(low.astype(jnp.float32), (half, width)),
            ],
            axis=0,
        ).astype(jnp.bfloat16)
        totals = list(totals)
        for s in range(point_count):
            cells = cell_rows(turn, s)
            spot = jnp.where(place_ids == narrow_rows(cells % (2 * depth), 2 * depth), one, zero)
            spots[turn, s] = spot
            weights = jnp.where(
                both_ids == narrow_rows(cells // (2 * depth), 2 * half), split, zero
            )
            for p in range(2):
                totals[p] = totals[p] + lax.dot_general(
                    weights,
                    spot[p * depth : (p + 1) * depth],
                    (((1,), (1,)), ((), ())),
                    preferred_element_type=jnp.float32,
                )
        return totals

    totals = [jnp.zeros((2 * half, depth), jnp.float32)] * 2
    first = turns // 2
    for turn in range(first):
        totals = deposit(turn, totals)

    loads[2].wait()
    loads[3].wait()
    for side, j in enumerate((0, cells_y - 1)):
        for k in range(3):
            for i in range(cells_x):
                flow_out_y[side, k * cells_x + i : k * cells_x + i + 1] = fluid_ref[k, i, j : j + 1]
            for side_x, i in enumerate((0, cells_x - 1)):
                flow_out_c[side_x * 2 + side, k : k + 1] = fluid_ref[k, i, j : j + 1]

    pl.semaphore_wait(barrier, len(DIRECTIONS))

    def flow_copy(slot):
        dx, dy = DIRECTIONS[slot]
        side_x, side_y = int(dx > 0), int(dy > 0)
        if dy == 0:
            source, target = fluid_ref.at[:, side_x * (cells_x - 1)], flow_in_x.at[side_x]
        elif dx == 0:
            source, target = flow_out_y.at[side_y], flow_in_y.at[side_y]
        else:
            corner = side_x * 2 + side_y
            source, target = flow_out_c.at[corner], flow_in_c.at[corner]
        return pltpu.make_async_remote_copy(
            src_ref=source,
            dst_ref=target,
            send_sem=send_sem.at[8 + slot],
            recv_sem=recv_sem.at[8 + slot],
            device_id=neighbour(DIRECTIONS[slot]),
            device_id_type=MESH,
        )

    def volume_copy(slot):
        dx, dy = DIRECTIONS[slot]
        side_x, side_y = int(dx > 0), int(dy > 0)
        if dy == 0:
            source, target = out_x.at[side_x], in_x.at[side_x]
        elif dx == 0:
            source, target = out_y.at[side_y], in_y.at[side_y]
        else:
            corner = side_x * 2 + side_y
            source, target = out_c.at[corner], in_c.at[corner]
        return pltpu.make_async_remote_copy(
            src_ref=source,
            dst_ref=target,
            send_sem=send_sem.at[slot],
            recv_sem=recv_sem.at[slot],
            device_id=neighbour(DIRECTIONS[slot]),
            device_id_type=MESH,
        )

    for slot in range(8):
        flow_copy(slot).start()

    for turn in range(first, turns):
        totals = deposit(turn, totals)
    evens, odds = pl.ds(0, half, stride=2), pl.ds(1, half, stride=2)
    tile[evens] = totals[0][:half] + totals[0][half:]
    tile[odds] = totals[1][:half] + totals[1][half:]

    band = 2 * wide_y
    top = (wide_x - 2) * wide_y
    out_x[0, :band] = tile[:band]
    out_x[1, :band] = tile[top : top + band]
    for side, j in enumerate((0, wide_y - 2)):
        for i in range(wide_x):
            out_y[side, 2 * i : 2 * i + 2] = tile[i * wide_y + j : i * wide_y + j + 2]
        for side_x, first_i in enumerate((0, wide_x - 2)):
            for step in range(2):
                start = (first_i + step) * wide_y + j
                out_c[side_x * 2 + side, 2 * step : 2 * step + 2] = tile[start : start + 2]

    for k in range(3):
        for i in range(cells_x):
            start = (i + 1) * wide_y + 1
            wide[k, start : start + cells_y] = fluid_ref[k, i]

    for slot in (4, 5, 6, 7, 0, 1, 2, 3):
        volume_copy(slot).start()

    spare = rows - wide_x * wide_y
    for k in range(3):
        if spare:
            wide[k, wide_x * wide_y :] = jnp.zeros((spare, depth), jnp.float32)
    for slot in range(8):
        flow_copy(slot).wait()
    for k in range(3):
        for side in range(2):
            i = wide_x - 1 if side == 0 else 0
            wide[k, i * wide_y + 1 : i * wide_y + 1 + cells_y] = flow_in_x[side, k]
            j = wide_y - 1 if side == 0 else 0
            for layer in range(cells_x):
                at = (layer + 1) * wide_y + j
                wide[k, at : at + 1] = flow_in_y[side, k * cells_x + layer : k * cells_x + layer + 1]
            for side_y in range(2):
                at = i * wide_y + (wide_y - 1 if side_y == 0 else 0)
                wide[k, at : at + 1] = flow_in_c[side * 2 + side_y, k : k + 1]

    for slot in range(8):
        volume_copy(slot).wait()
    tile[top : top + band] += in_x[0, :band]
    tile[:band] += in_x[1, :band]
    for side in range(2):
        j = wide_y - 2 if side == 0 else 0
        for i in range(wide_x):
            tile[i * wide_y + j : i * wide_y + j + 2] += in_y[side, 2 * i : 2 * i + 2]
        for side_x in range(2):
            first_i = wide_x - 2 if side_x == 0 else 0
            for step in range(2):
                start = (first_i + step) * wide_y + j
                tile[start : start + 2] += in_c[side_x * 2 + side, 2 * step : 2 * step + 2]

    void = jnp.maximum(1.0 - tile[...], void_floor)
    tile[...] = void
    void = jnp.concatenate([tile[evens], tile[odds]], axis=1)
    resistance = jnp.exp(exponent * jnp.log(void))
    parts = [
        resistance * jnp.concatenate([wide[k, evens], wide[k, odds]], axis=1) for k in range(3)
    ] + [resistance]
    mixed = jnp.concatenate(
        [part[g * 8 : (g + 1) * 8] for g in range(half // 8) for part in parts], axis=0
    )
    high, low = halves(mixed)
    fields[: 4 * half] = high
    fields[4 * half :] = low
    for i in range(cells_x):
        start = (i + 1) * wide_y + 1
        void_ref[i] = tile[start : start + cells_y]

    group_ids = lax.broadcasted_iota(jnp.int32, (8, width), 0)
    for turn in range(turns):
        sums = [jnp.zeros((8, width), jnp.float32) for _ in range(4)]
        for s in range(point_count):
            spot = spots[turn, s]
            picked = jnp.dot(fields[...], spot, preferred_element_type=jnp.float32)
            row = jnp.broadcast_to(cell_rows(turn, s) // (2 * depth), (8, width))
            for g in range(half // 8):
                hit = row == group_ids + 8 * g
                for k in range(4):
                    at = (g * 4 + k) * 8
                    value = picked[at : at + 8] + picked[4 * half + at : 4 * half + at + 8]
                    sums[k] = sums[k] + jnp.where(hit, value, 0.0)
        share = shares(turn)
        weight_sum = jnp.sum(sums[3], axis=0, keepdims=True)
        for k in range(3):
            pulling = jnp.sum(sums[k], axis=0, keepdims=True)
            for h in range(pair):
                at = slice(h * lanes, (h + 1) * lanes)
                block = turn * pair + h
                drag_ref[k, block : block + 1] = (
                    drag_scale
                    * share[:, at]
                    * (pulling[:, at] - velocity_ref[k, block : block + 1] * weight_sum[:, at])
                )


def body(fluid_velocity, particle_velocity, particle_volume, satellite_cells, live_blocks):
    _, cells_x, cells_y, depth = fluid_velocity.shape
    wide_x, wide_y = cells_x + 2, cells_y + 2
    satellites = satellite_cells[0, 0]
    block_count, point_count, lanes = satellites.shape
    pair = 2 if block_count % 2 == 0 else 1
    rows = rounded_up(wide_x * wide_y, 16)
    band = rounded_up(2 * wide_y, 8)
    sides = rounded_up(2 * wide_x, 8)
    flow_sides = rounded_up(3 * cells_x, 8)
    sizes = (lax.axis_size("gx"), lax.axis_size("gy"), cells_x, cells_y, pair, point_count)
    vmem = pl.BlockSpec(memory_space=pltpu.VMEM)
    f32 = jnp.float32
    void_fraction, drag = pl.pallas_call(
        functools.partial(kernel, sizes),
        out_shape=(
            pltpu.VMEM((cells_x, cells_y, depth), f32),
            pltpu.VMEM((3, block_count, lanes), f32),
        ),
        in_specs=[vmem] + [pl.BlockSpec(memory_space=pltpu.HBM)] * 4,
        out_specs=(vmem, vmem),
        scratch_shapes=[
            pltpu.VMEM(fluid_velocity.shape, f32),
            pltpu.VMEM((3, block_count, lanes), f32),
            pltpu.VMEM((block_count, lanes), f32),
            pltpu.VMEM((point_count, block_count, lanes), jnp.int32),
            pltpu.SemaphoreType.DMA((4,)),
            pltpu.VMEM((block_count // pair, point_count, 2 * depth, pair * lanes), jnp.bfloat16),
            pltpu.VMEM((rows, depth), f32),
            pltpu.VMEM((3, rows, depth), f32),
            pltpu.VMEM((4 * rows, 2 * depth), jnp.bfloat16),
            pltpu.VMEM((2, band, depth), f32),
            pltpu.VMEM((2, sides, depth), f32),
            pltpu.VMEM((4, 8, depth), f32),
            pltpu.VMEM((2, band, depth), f32),
            pltpu.VMEM((2, sides, depth), f32),
            pltpu.VMEM((4, 8, depth), f32),
            pltpu.VMEM((2, flow_sides, depth), f32),
            pltpu.VMEM((4, 8, depth), f32),
            pltpu.VMEM((2, 3, cells_y, depth), f32),
            pltpu.VMEM((2, flow_sides, depth), f32),
            pltpu.VMEM((4, 8, depth), f32),
            pltpu.SemaphoreType.DMA((16,)),
            pltpu.SemaphoreType.DMA((16,)),
        ],
        compiler_params=pltpu.CompilerParams(
            collective_id=0, has_side_effects=True
        ),
    )(
        live_blocks,
        fluid_velocity,
        jnp.swapaxes(particle_velocity[0, 0], 0, 1),
        particle_volume[0, 0],
        jnp.swapaxes(satellites, 0, 1),
    )
    return void_fraction, jnp.swapaxes(drag, 0, 1)[None, None]


def solution(mesh):
    placed = (
        P(None, "gx", "gy", None),
        P("gx", "gy", None, None, None),
        P("gx", "gy", None, None),
        P("gx", "gy", None, None, None),
        P("gx", "gy"),
    )
    return jax.shard_map(
        body,
        mesh=mesh,
        in_specs=placed,
        out_specs=(P("gx", "gy", None), P("gx", "gy", None, None, None)),
        check_vma=False,
    )
```
